32 devices in a mesh: rows: 2 (over core), cols: 4 (over y, x), slabs: 4 (over z).
Axes of the slice: x: 2, y: 2, z: 4, core: 2. Of those that a mesh axis runs over, the one named last changes fastest.
Arguments:
- field_now: float32 [8, 128, 512, 128], P('rows', 'cols', 'slabs'), may hold values from 0.5 to 2
- earlier: float32 [8, 128, 512, 128], P('rows', 'cols', 'slabs'), may hold values from 0.2 to 1.8
- speed_square: float32 [8, 128, 512, 128], P('rows', 'cols', 'slabs'), may hold values from 0.05 to 0.3
Outputs:
- scaled_field: float32 [8, 128, 512, 128], P('rows', 'cols', 'slabs')
- field_now_end: float32 [8, 128, 512, 128], P('rows', 'cols', 'slabs')
The draws below stay inside these ranges and needn't reach their ends.
All inputs are finite; a program needn't handle non-finite values.
Results may differ from the reference program's by a relative error of at most 0.00002.
Values sent between devices are 32-bit elements; how exact they have to be, the bound alone decides.
A program may use at most 128 MiB of HBM per device.

```python
import jax
import jax.numpy as jnp
from jax import lax

GRID_J = 8
GRID_I = 128
GRID_K = 512
MEMBERS = 128
STEPS = 3


def block_levels(rng, shape, cuts, smallest, top_value):
    level, own = 1.0, jax.random.fold_in(rng, 6)
    for position, blocks in cuts:
        steps = jnp.exp(jax.random.uniform(jax.random.fold_in(own, position), (blocks,), jnp.float32, smallest / len(cuts), top_value / len(cuts)))
        level = level * jnp.repeat(steps, shape[position] // blocks).reshape([-1 if axis == position else 1 for axis in range(len(shape))])
    return level


def setup_inputs(seed: int = 0) -> dict:
    keys = jax.random.split(jax.random.key(seed), 4)
    field_now = jnp.clip(0.5 + 1.5 * jax.random.uniform(keys[0], (GRID_J, GRID_I, GRID_K, MEMBERS), jnp.float32) ** block_levels(keys[0], (GRID_J, GRID_I, GRID_K, MEMBERS), ((0, 2), (1, 4), (2, 4)), -0.2, 0.2), 0.5, 2.0)
    earlier = jnp.clip(0.2 + 1.5999999 * jax.random.uniform(keys[1], (GRID_J, GRID_I, GRID_K, MEMBERS), jnp.float32) ** block_levels(keys[1], (GRID_J, GRID_I, GRID_K, MEMBERS), ((0, 2), (1, 4), (2, 4)), -0.2, 0.2), 0.2, 1.8)
    speed_square = jnp.clip(0.05 + 0.25 * jax.random.uniform(keys[2], (GRID_J, GRID_I, GRID_K, MEMBERS), jnp.float32) ** block_levels(keys[2], (GRID_J, GRID_I, GRID_K, MEMBERS), ((0, 2), (1, 4), (2, 4)), -0.2, 0.2), 0.05, 0.3)
    return {"field_now": field_now, "earlier": earlier, "speed_square": speed_square}


def without_rim(values, dims):
    for dim in dims:
        values = lax.slice_in_dim(values, 1, values.shape[dim] - 1, axis=dim)
    return values

def shifted_cells(values, dim, start, dims):
    others = [other for other in dims if other != dim]
    values = without_rim(values, others)
    return lax.slice_in_dim(values, start, start + values.shape[dim] - 2, axis=dim)

def march_step(padded, before, speed_square):
    middle = without_rim(padded, (0, 1, 2))
    lower = [shifted_cells(padded, dim, 0, (0, 1, 2)) for dim in (0, 1, 2)]
    upper = [shifted_cells(padded, dim, 2, (0, 1, 2)) for dim in (0, 1, 2)]
    spread = lower[0] + upper[0] + lower[1] + upper[1] + lower[2] + upper[2] - 6.0 * middle
    return 2.0 * middle - before + speed_square * spread

def reference(field_now, earlier, speed_square):
    for step in range(STEPS):
        later = march_step(jnp.pad(field_now, ((1, 1), (1, 1), (1, 1), (0, 0)), mode='constant'), earlier, speed_square)
        earlier, field_now = (field_now, later)
    line_mean = lax.optimization_barrier(jnp.mean(field_now, axis=2, keepdims=True))
    centred = field_now - line_mean
    line_variance = lax.optimization_barrier(jnp.mean(centred * centred, axis=2, keepdims=True))
    scaled_field = centred * lax.rsqrt(line_variance + 0.0001)
    return (scaled_field, field_now)
```

```python
import functools

import jax
import jax.numpy as jnp
from jax import lax
from jax.experimental import pallas as pl
from jax.experimental.pallas import tpu as pltpu
from jax.sharding import PartitionSpec as P

STEPS = 3
EPS = 1e-4
MESH = pl.DeviceIdType.MESH
AXES = ("rows", "cols", "slabs")


def march_kernel(
    counts, relay, now_hbm, old_hbm, speed_hbm, field, mean_ref, scale_ref,
    work, speed, face_out, face_in, own_stats, own_edge, in_stats, all_edge,
    relayed, load_x, load_y, load_c, send_sem, recv_sem, half_send, half_recv,
    pass_send, pass_recv, stat_send, stat_recv, edge_send, edge_recv,
):
    nj, ni, nk, lanes = now_hbm.shape
    n_slabs = counts["slabs"]
    parts = speed_parts(ni)
    width = ni // parts
    here = {axis: lax.axis_index(axis) for axis in AXES}
    has_low = {axis: here[axis] > 0 for axis in AXES}
    has_high = {axis: here[axis] < counts[axis] - 1 for axis in AXES}

    inner = (pl.ds(1, nj), pl.ds(1, ni))
    copy_x = pltpu.make_async_copy(now_hbm, work.at[inner], load_x)
    copy_x.start()
    copies = []
    for part in range(parts):
        span, padded = pl.ds(part * width, width), pl.ds(1 + part * width, width)
        copies.append((
            pltpu.make_async_copy(old_hbm.at[:, span], field.at[pl.ds(1, nj), padded], load_y.at[part]),
            pltpu.make_async_copy(speed_hbm.at[:, span], speed.at[:, span], load_c.at[part]),
        ))
        for copy in copies[-1]:
            copy.start()

    barrier = pltpu.get_barrier_semaphore()
    expected = jnp.int32(n_slabs - 1)
    for axis in ("rows", "cols"):
        for there, shift in ((has_low[axis], -1), (has_high[axis], 1)):
            expected = expected + there.astype(jnp.int32)

            @pl.when(there)
            def _():
                pl.semaphore_signal(barrier, inc=1, device_id={axis: here[axis] + shift}, device_id_type=MESH)

    peers = [lax.rem(here["slabs"] + gap, n_slabs) for gap in range(1, n_slabs)]
    for peer in peers:
        pl.semaphore_signal(barrier, inc=1, device_id={"slabs": peer}, device_id_type=MESH)
    if relay:
        over = lax.rem(here["cols"] + 2, 4)
        pl.semaphore_signal(barrier, inc=1, device_id={"cols": over}, device_id_type=MESH)
        expected = expected + 1
    pl.semaphore_wait(barrier, expected)

    half = nj // 2 if relay else 0

    def half_copy(step, to_high, kind):
        buffer = work if step % 2 == 0 else field
        edge = ni - 1 if to_high else 0
        source = now_hbm.at[pl.ds(0, half), edge] if step == 0 else buffer.at[pl.ds(1, half), edge + 1]
        landing = buffer.at[pl.ds(1, half), 0 if to_high else ni + 1]
        sems = half_send.at[step, int(to_high)], half_recv.at[step, int(to_high)]
        target = here["cols"] + (1 if to_high else -1)
        if kind == "to":
            landing, target = relayed.at[step], over
            sems = sems[0], pass_recv.at[step]
        elif kind == "on":
            source, target = relayed.at[step], here["cols"] + (-1 if to_high else 1)
            sems = pass_send.at[step], sems[1]
        return pltpu.make_async_remote_copy(
            source, landing, *sems, device_id={"cols": target}, device_id_type=MESH
        )

    def halves(step, what):
        if not relay:
            return
        me = here["cols"]
        for to_high, source, target in ((True, 1, 2), (False, 2, 1)):
            edge_sends = (me == 0) | (me == 2) if to_high else (me == 1) | (me == 3)
            if what == "start":
                pl.when(me == source)(half_copy(step, to_high, "to").start)
                pl.when(edge_sends)(half_copy(step, to_high, "straight").start)
            elif what == "pass":
                @pl.when(me == (3 if to_high else 0))
                def _():
                    half_copy(step, to_high, "to").wait_recv()
                    half_copy(step, to_high, "on").start()
            elif what == "sent":
                pl.when(has_high["cols"] if to_high else has_low["cols"])(
                    half_copy(step, to_high, "straight").wait_send
                )
                pl.when(me == (3 if to_high else 0))(half_copy(step, to_high, "on").wait_send)
            else:
                pl.when(has_low["cols"] if to_high else has_high["cols"])(
                    half_copy(step, to_high, "straight").wait_recv
                )

    def face_copy(step, axis, to_high):
        buffer = work if step % 2 == 0 else field
        number = 2 * AXES.index(axis) + int(to_high)
        target = here[axis] + (1 if to_high else -1)
        if axis == "slabs":
            source, landing = face_out.at[step, int(to_high)], face_in.at[step, int(to_high)]
        elif axis == "cols":
            edge = ni - 1 if to_high else 0
            rest = pl.ds(half, nj - half)
            source = now_hbm.at[rest, edge] if step == 0 else buffer.at[pl.ds(1 + half, nj - half), edge + 1]
            landing = buffer.at[pl.ds(1 + half, nj - half), 0 if to_high else ni + 1]
        else:
            edge = nj - 1 if to_high else 0
            source = now_hbm.at[edge] if step == 0 else buffer.at[edge + 1, pl.ds(1, ni)]
            landing = buffer.at[0 if to_high else nj + 1, pl.ds(1, ni)]
        return pltpu.make_async_remote_copy(
            source, landing, send_sem.at[step, number], recv_sem.at[step, number],
            device_id={axis: target}, device_id_type=MESH,
        )

    def exchange(step, axis, what):
        if axis == "cols":
            halves(step, what)
        for to_high in (False, True):
            sends = has_high[axis] if to_high else has_low[axis]
            takes = has_low[axis] if to_high else has_high[axis]
            copy = face_copy(step, axis, to_high)
            if what == "start":
                pl.when(sends)(copy.start)
            elif what == "sent":
                pl.when(sends)(copy.wait_send)
            else:
                pl.when(takes)(copy.wait_recv)

    exchange(0, "cols", "start")
    exchange(0, "rows", "start")

    zeros_line = jnp.zeros((nk, lanes), jnp.float32)
    for buffer in (work, field):
        for absent, edge in ((~has_low["rows"], 0), (~has_high["rows"], nj + 1)):
            @pl.when(absent)
            def _():
                @pl.loop(1, ni + 1)
                def _(i):
                    buffer[edge, i] = zeros_line
        for absent, edge in ((~has_low["cols"], 0), (~has_high["cols"], ni + 1)):
            @pl.when(absent)
            def _():
                @pl.loop(1, nj + 1)
                def _(j):
                    buffer[j, edge] = zeros_line
    for absent, side in ((~has_low["slabs"], 1), (~has_high["slabs"], 0)):
        @pl.when(absent)
        def _():
            for step in range(STEPS):
                face_in[step, side] = jnp.zeros((nj, ni, lanes), jnp.float32)
    own_stats[...] = jnp.zeros_like(own_stats)

    copy_x.wait()

    @pl.loop(0, ni)
    def _(i):
        for j in range(nj):
            face_out[0, 0, j, pl.ds(i, 1), :] = work[j + 1, i + 1, pl.ds(0, 1), :]
            face_out[0, 1, j, pl.ds(i, 1), :] = work[j + 1, i + 1, pl.ds(nk - 1, 1), :]

    exchange(0, "slabs", "start")

    groups = nk // 8
    row_number = lax.broadcasted_iota(jnp.int32, (8, lanes), 0)

    def line(step, i, edge_side=None):
        now, old = (work, field) if step % 2 == 1 else (field, work)
        last = step == STEPS
        sums = [None] * nj
        for g in range(groups):
            k = pl.ds(8 * g, 8)
            column = [now[j, i, k, :] for j in range(nj + 2)]
            for j in range(1, nj + 1):
                middle = column[j]
                if g == 0:
                    low = jnp.where(
                        row_number == 0,
                        jnp.broadcast_to(face_in[step - 1, 1, j - 1, pl.ds(i - 1, 1), :], (8, lanes)),
                        pltpu.roll(middle, 1, 0),
                    )
                else:
                    low = now[j, i, pl.ds(8 * g - 1, 8), :]
                if g == groups - 1:
                    high = jnp.where(
                        row_number == 7,
                        jnp.broadcast_to(face_in[step - 1, 0, j - 1, pl.ds(i - 1, 1), :], (8, lanes)),
                        pltpu.roll(middle, 7, 0),
                    )
                else:
                    high = now[j, i, pl.ds(8 * g + 1, 8), :]
                spread = (
                    (column[j - 1] + column[j + 1])
                    + (now[j, i - 1, k, :] + now[j, i + 1, k, :])
                    + (low + high)
                    - 6.0 * middle
                )
                later = 2.0 * middle - old[j, i, k, :] + speed[j - 1, i - 1, k, :] * spread
                old[j, i, k, :] = later
                if last:
                    sums[j - 1] = later if g == 0 else sums[j - 1] + later
                else:
                    if g == 0:
                        face_out[step, 0, j - 1, pl.ds(i - 1, 1), :] = later[0:1]
                    if g == groups - 1:
                        face_out[step, 1, j - 1, pl.ds(i - 1, 1), :] = later[7:8]
        if last:
            for j in range(nj):
                total = jnp.sum(sums[j], axis=0, keepdims=True)
                mean = jnp.broadcast_to(total * (1.0 / nk), (8, lanes))
                squares = None
                for g in range(groups):
                    moved = old[j + 1, i, pl.ds(8 * g, 8), :] - mean
                    squares = moved * moved if g == 0 else squares + moved * moved
                square = jnp.sum(squares, axis=0, keepdims=True)
                if edge_side is None:
                    own_stats[0, 0, j, pl.ds(i - 1, 1), :] = total
                    own_stats[0, 1, j, pl.ds(i - 1, 1), :] = square
                else:
                    own_edge[0, pl.ds(edge_side * nj + j, 1), :] = total
                    own_edge[1, pl.ds(edge_side * nj + j, 1), :] = square

    def lines(step, start, stop):
        @pl.loop(start, stop)
        def _(i):
            line(step, i)

    levels = n_slabs.bit_length() - 1
    partners = []
    for level in range(levels):
        bit = lax.rem(here["slabs"] // 2**level, 2)
        partners.append(here["slabs"] + (1 - 2 * bit) * 2**level)

    def stat_copy(part, level):
        rows = pl.ds(part * width, width)
        return pltpu.make_async_remote_copy(
            own_stats.at[level, :, :, rows], in_stats.at[level, :, :, rows],
            stat_send.at[part, level], stat_recv.at[part, level],
            device_id={"slabs": partners[level]}, device_id_type=MESH,
        )

    def edge_copy(gap):
        return pltpu.make_async_remote_copy(
            own_edge, all_edge.at[gap - 1], edge_send.at[gap - 1], edge_recv.at[gap - 1],
            device_id={"slabs": peers[gap - 1]}, device_id_type=MESH,
        )

    def merged(part, level):
        rows = pl.ds(part * width, width)
        stat_copy(part, level).wait_recv()
        mine, theirs = own_stats[level, :, :, rows, :], in_stats[level, :, :, rows, :]
        cells = float(nk * 2**level)
        apart = (theirs[0] - mine[0]) * (1.0 / cells)
        return mine[0] + theirs[0], mine[1] + theirs[1] + (0.5 * cells) * apart * apart

    def advance(part, level):
        rows = pl.ds(part * width, width)
        total, square = merged(part, level)
        own_stats[level + 1, 0, :, rows, :] = total
        own_stats[level + 1, 1, :, rows, :] = square
        stat_copy(part, level + 1).start()

    gaps = range(1, n_slabs)
    for step in range(1, STEPS + 1):
        if step == 3:
            for axis in AXES:
                exchange(1, axis, "sent")
        exchange(step - 1, "rows", "taken")
        exchange(step - 1, "slabs", "taken")
        for part in range(parts):
            if step == 1:
                for copy in copies[part]:
                    copy.wait()
            start, stop = 1 + part * width, 1 + (part + 1) * width
            lines(step, max(start, 2), min(stop, ni))
            if part == 0:
                halves(step - 1, "pass")
            if step == STEPS:
                stat_copy(part, 0).start()
                if part >= 2 and levels > 1:
                    advance(part - 2, 0)
        if step == STEPS and levels > 1:
            for part in range(max(parts - 2, 0), parts):
                advance(part, 0)
        exchange(step - 1, "cols", "taken")
        line(step, 1, 0)
        line(step, ni, 1)
        if step < STEPS:
            for axis in ("cols", "slabs", "rows"):
                exchange(step, axis, "start")
    for gap in gaps:
        edge_copy(gap).start()
    for level in range(1, levels - 1):
        for part in range(parts):
            advance(part, level)

    whole = float(nk * n_slabs)

    def combine(own, others):
        mean = own[0]
        for other in others:
            mean = mean + other[0]
        mean = mean * (1.0 / whole)
        square = None
        for one in (own, *others):
            gap = one[0] * (1.0 / nk) - mean
            term = one[1] + nk * gap * gap
            square = term if square is None else square + term
        return mean, lax.rsqrt(square * (1.0 / whole) + EPS)

    for part in range(parts):
        rows = pl.ds(part * width, width)
        total, square = merged(part, levels - 1)
        mean_ref[:, rows, :] = total * (1.0 / whole)
        scale_ref[:, rows, :] = lax.rsqrt(square * (1.0 / whole) + EPS)
    for gap in gaps:
        edge_copy(gap).wait_recv()
    mean, scale = combine(own_edge[...], [all_edge[gap - 1] for gap in gaps])
    for side, i in ((0, 0), (1, ni - 1)):
        for j in range(nj):
            place = side * nj + j
            mean_ref[j, pl.ds(i, 1), :] = mean[place:place + 1]
            scale_ref[j, pl.ds(i, 1), :] = scale[place:place + 1]

    for step in range(STEPS):
        if step != 1:
            for axis in AXES:
                exchange(step, axis, "sent")
    for part in range(parts):
        for level in range(levels):
            stat_copy(part, level).wait_send()
    for gap in gaps:
        edge_copy(gap).wait_send()


def speed_parts(ni):
    return 4 if ni % 32 == 0 else 1


def scale_kernel(field, mean_ref, scale_ref, scaled_hbm, field_hbm, scaled, out_sem, field_sem):
    nj, ni, nk, lanes = scaled_hbm.shape
    parts = speed_parts(ni)
    width = ni // parts
    field_copies = [
        pltpu.make_async_copy(field.at[j + 1, pl.ds(1, ni)], field_hbm.at[j], field_sem.at[j])
        for j in range(nj)
    ]
    out_copies = []
    for j in range(nj):
        for part in range(parts):
            @pl.loop(part * width, (part + 1) * width)
            def _(i):
                mean = jnp.broadcast_to(mean_ref[j, pl.ds(i, 1), :], (8, lanes))
                scale = jnp.broadcast_to(scale_ref[j, pl.ds(i, 1), :], (8, lanes))
                for g in range(nk // 8):
                    k = pl.ds(8 * g, 8)
                    scaled[j, i, k, :] = (field[j + 1, i + 1, k, :] - mean) * scale

            rows = pl.ds(part * width, width)
            copy = pltpu.make_async_copy(
                scaled.at[j, rows], scaled_hbm.at[j, rows], out_sem.at[j, part]
            )
            copy.start()
            out_copies.append(copy)
            if part == 0:
                field_copies[j].start()
    for copy in (*field_copies, *out_copies):
        copy.wait()


def shards(counts, relay, field_now, earlier, speed_square):
    nj, ni, nk, lanes = field_now.shape
    n_slabs = counts["slabs"]
    levels = n_slabs.bit_length() - 1
    assert n_slabs == 2**levels and levels >= 1
    relay = relay and nj > 1
    parts = speed_parts(ni)
    f32 = jnp.float32
    padded = (nj + 2, ni + 2, nk, lanes)
    hbm = pl.BlockSpec(memory_space=pltpu.HBM)
    vmem = pl.BlockSpec(memory_space=pltpu.VMEM)
    cells = nj * ni * nk * lanes
    dma = pltpu.SemaphoreType.DMA
    field, mean, scale = pl.pallas_call(
        functools.partial(march_kernel, counts, relay),
        name="march",
        out_shape=(
            pltpu.VMEM(padded, f32),
            pltpu.VMEM((nj, ni, lanes), f32),
            pltpu.VMEM((nj, ni, lanes), f32),
        ),
        in_specs=[hbm] * 3,
        out_specs=(vmem,) * 3,
        scratch_shapes=[
            pltpu.VMEM(padded, f32),
            pltpu.VMEM((nj, ni, nk, lanes), f32),
            pltpu.VMEM((STEPS, 2, nj, ni, lanes), f32),
            pltpu.VMEM((STEPS, 2, nj, ni, lanes), f32),
            pltpu.VMEM((levels, 2, nj, ni, lanes), f32),
            pltpu.VMEM((2, 2 * nj, lanes), f32),
            pltpu.VMEM((levels, 2, nj, ni, lanes), f32),
            pltpu.VMEM((n_slabs - 1, 2, 2 * nj, lanes), f32),
            pltpu.VMEM((STEPS, max(nj // 2, 1), nk, lanes), f32),
            dma(()),
            dma((parts,)),
            dma((parts,)),
            dma((STEPS, 6)),
            dma((STEPS, 6)),
            dma((STEPS, 2)),
            dma((STEPS, 2)),
            dma((STEPS,)),
            dma((STEPS,)),
            dma((parts, levels)),
            dma((parts, levels)),
            dma((n_slabs - 1,)),
            dma((n_slabs - 1,)),
        ],
        compiler_params=pltpu.CompilerParams(
            collective_id=0, has_side_effects=True, vmem_limit_bytes=45 * 2**20
        ),
        cost_estimate=pl.CostEstimate(flops=33 * cells, bytes_accessed=12 * cells, transcendentals=0),
    )(field_now, earlier, speed_square)
    return pl.pallas_call(
        scale_kernel,
        name="scale",
        out_shape=(jax.ShapeDtypeStruct(field_now.shape, f32),) * 2,
        in_specs=[vmem] * 3,
        out_specs=(hbm,) * 2,
        scratch_shapes=[
            pltpu.VMEM((nj, ni, nk, lanes), f32),
            dma((nj, parts)),
            dma((nj,)),
        ],
        compiler_params=pltpu.CompilerParams(vmem_limit_bytes=16 * 2**20),
        cost_estimate=pl.CostEstimate(flops=2 * cells, bytes_accessed=8 * cells, transcendentals=0),
    )(field, mean, scale)


def crosses(mesh):
    order = ("rows", "cols", "slabs")
    devices = mesh.devices.transpose([mesh.axis_names.index(axis) for axis in order])
    if devices.shape[1] != 4:
        return False
    one, other = (getattr(devices[0, place, 0], "coords", None) for place in (1, 2))
    return one is not None and sum(a != b for a, b in zip(one, other)) > 1


def solution(mesh):
    spec = P("rows", "cols", "slabs", None)
    return jax.shard_map(
        functools.partial(shards, dict(mesh.shape), crosses(mesh)),
        mesh=mesh,
        in_specs=(spec,) * 3,
        out_specs=(spec,) * 2,
        check_vma=False,
    )
```
